32 devices in a mesh: replica: 2 (over core), model: 4 (over y, x), shift: 4 (over z).
Axes of the slice: x: 2, y: 2, z: 4, core: 2. Of those that a mesh axis runs over, the one named last changes fastest.
Arguments:
- partial_gate: float32 [8, 1024, 3072], P(('shift', 'replica'), None, 'model'), parts along dimension 0, may hold values from -0.875 to 0.875
- partial_up: float32 [8, 1024, 3072], P(('shift', 'replica'), None, 'model'), parts along dimension 0, may hold values from -0.875 to 0.875
- partial_down: float32 [8, 3072, 1024], P(('shift', 'replica'), 'model'), parts along dimension 0, may hold values from -0.875 to 0.875
- partial_norm: float32 [8, 1024], P(('shift', 'replica')), parts along dimension 0, may hold values from -8 to 8
- master_gate: float32 [4096, 3072], P(('shift', 'replica'), 'model'), parts along dimension 0, may hold values from -0.25 to 0.25
- master_up: float32 [4096, 3072], P(('shift', 'replica'), 'model'), parts along dimension 0, may hold values from -0.25 to 0.25
- master_down: float32 [12288, 1024], P(('shift', 'model'), 'replica'), parts along dimension 0, may hold values from -0.15625 to 0.15625
- master_norm: float32 [4096], P(('shift', 'replica')), parts along dimension 0, may hold values from 0.25 to 1.75
- memory_gate: float32 [4096, 3072], P(('shift', 'replica'), 'model'), parts along dimension 0, may hold values from -0.1875 to 0.1875
- memory_up: float32 [4096, 3072], P(('shift', 'replica'), 'model'), parts along dimension 0, may hold values from -0.1875 to 0.1875
- memory_down: float32 [12288, 1024], P(('shift', 'model'), 'replica'), parts along dimension 0, may hold values from -0.109375 to 0.109375
- memory_norm: float32 [4096], P(('shift', 'replica')), parts along dimension 0, may hold values from -1.75 to 1.75
Outputs:
- compute_gate: bfloat16 [4096, 3072], P('shift', 'model'), parts along dimension 0
- compute_up: bfloat16 [4096, 3072], P('shift', 'model'), parts along dimension 0
- compute_down: bfloat16 [12288, 1024], P(('shift', 'model')), parts along dimension 0
- compute_norm: bfloat16 [4096], P('shift'), parts along dimension 0
- stepped_gate: float32 [4096, 3072], P(('shift', 'replica'), 'model'), parts along dimension 0
- stepped_up: float32 [4096, 3072], P(('shift', 'replica'), 'model'), parts along dimension 0
- stepped_down: float32 [12288, 1024], P(('shift', 'model'), 'replica'), parts along dimension 0
- stepped_norm: float32 [4096], P(('shift', 'replica')), parts along dimension 0
- state_new_gate: float32 [4096, 3072], P(('shift', 'replica'), 'model'), parts along dimension 0
- state_new_up: float32 [4096, 3072], P(('shift', 'replica'), 'model'), parts along dimension 0
- state_new_down: float32 [12288, 1024], P(('shift', 'model'), 'replica'), parts along dimension 0
- state_new_norm: float32 [4096], P(('shift', 'replica')), parts along dimension 0
The draws below stay inside these ranges and needn't reach their ends.
There are 4 independent parts, one for each index of `shift`. The reference program is written for one: setup_inputs(seed, part) draws one part's arguments, and reference() takes and returns one part's arrays. A program takes and returns all parts, laid end to end along the dimension named above; each array names one. Nothing has to cross between parts.
All inputs are finite; a program needn't handle non-finite values.
Results may differ from the reference program's by a relative error of at most 0.001.
Values may be sent and summed in bfloat16 or wider, within the bound.
A program may use at most 128 MiB of HBM per device.

```python
import jax
import jax.numpy as jnp
from jax import lax

WIDTH = 1024
INNER = 3072
REPLICAS = 2


def spiked(drawn, own_key, source, target, parts, factor):
    owner, partner = [(jnp.arange(drawn.shape[axis_at]) // (drawn.shape[axis_at] // parts)).reshape([-1 if axis == axis_at else 1 for axis in range(drawn.ndim)]) for axis_at in (source, target)]
    chosen = jax.random.permutation(own_key, parts)[partner]
    strong = (owner == chosen) | (owner == (partner + parts // 2) % parts)
    return jnp.where(strong, factor * drawn, drawn)


def steps_of(stream_key, dims, cuts, smallest, high):
    def one(position, blocks):
        steps = jax.random.uniform(jax.random.fold_in(jax.random.fold_in(stream_key, 6), position), (blocks,), jnp.float32, smallest / len(cuts), high / len(cuts))
        return jnp.repeat(jnp.exp(steps), dims[position] // blocks).reshape((-1,) + (1,) * (len(dims) - position - 1))

    loudness = one(*cuts[0])
    for cut in cuts[1:]:
        loudness = loudness * one(*cut)
    return loudness


def scatter_about(key, dims, deviation, most, pieces=(), dtype=jnp.bfloat16):
    factor_of = steps_of(key, dims, pieces, -0.22, 0.18) if pieces else 1.0
    values = jax.random.normal(key, dims, jnp.float32) * deviation * factor_of
    return jnp.minimum(jnp.maximum(values, -most), most).astype(dtype)


def noise_with(key, dims, scale, limit, split, heavy, kind=jnp.bfloat16):
    entries = scale * jax.random.normal(key, dims, jnp.float32)
    if split:
        entries = entries * steps_of(key, dims, split, -0.22, 0.18)
    return jnp.clip(spiked(entries, jax.random.fold_in(key, 3), *heavy), -limit, limit).astype(kind)


def setup_inputs(seed: int = 0, part: int = 0) -> dict:
    keys = jax.random.split(jax.random.key(seed), 13)
    part_splits = jax.random.split(jax.random.fold_in(keys[12], part), 13)
    partial_gate = noise_with(part_splits[0], (REPLICAS, WIDTH, INNER), 0.1, 0.875, ((0, 2), (2, 4)), (0, 1, 2, 2.0), jnp.float32)
    partial_up = noise_with(part_splits[1], (REPLICAS, WIDTH, INNER), 0.1, 0.875, ((0, 2), (2, 4)), (0, 1, 2, 2.0), jnp.float32)
    partial_down = noise_with(part_splits[2], (REPLICAS, INNER, WIDTH), 0.1, 0.875, ((0, 2), (1, 4)), (0, 2, 2, 2.0), jnp.float32)
    partial_norm = noise_with(part_splits[3], (REPLICAS, WIDTH), 1.0, 8.0, ((0, 2),), (0, 1, 2, 2.0), jnp.float32)
    master_gate = noise_with(part_splits[4], (WIDTH, INNER), WIDTH ** -0.5, 0.25, ((0, 2), (1, 4)), (1, 0, 4, 2.0), jnp.float32)
    master_up = noise_with(part_splits[5], (WIDTH, INNER), WIDTH ** -0.5, 0.25, ((0, 2), (1, 4)), (1, 0, 4, 2.0), jnp.float32)
    master_down = noise_with(part_splits[6], (INNER, WIDTH), INNER ** -0.5, 0.15625, ((0, 4), (1, 2)), (0, 1, 4, 2.0), jnp.float32)
    master_norm = jnp.clip(1.0 + 0.15 * jax.random.normal(part_splits[7], (WIDTH,), jnp.float32), 0.25, 1.75)
    memory_gate = scatter_about(part_splits[8], (WIDTH, INNER), WIDTH ** -0.5, 0.1875, ((0, 2), (1, 4)), jnp.float32)
    memory_up = scatter_about(part_splits[9], (WIDTH, INNER), WIDTH ** -0.5, 0.1875, ((0, 2), (1, 4)), jnp.float32)
    memory_down = scatter_about(part_splits[10], (INNER, WIDTH), INNER ** -0.5, 0.109375, ((0, 4), (1, 2)), jnp.float32)
    memory_norm = scatter_about(part_splits[11], (WIDTH,), 0.3, 1.75, ((0, 2),), jnp.float32)
    return {"partial_gate": partial_gate, "partial_up": partial_up, "partial_down": partial_down, "partial_norm": partial_norm, "master_gate": master_gate, "master_up": master_up, "master_down": master_down, "master_norm": master_norm, "memory_gate": memory_gate, "memory_up": memory_up, "memory_down": memory_down, "memory_norm": memory_norm}


learn_rate = 0.5
hold_rate = 0.9

def reference(partial_gate, partial_up, partial_down, partial_norm, master_gate, master_up, master_down, master_norm, memory_gate, memory_up, memory_down, memory_norm):
    mean_gate = lax.optimization_barrier(jnp.sum(partial_gate.astype(jnp.float32), axis=0)) * REPLICAS ** (-0.5)
    mean_up = lax.optimization_barrier(jnp.sum(partial_up.astype(jnp.float32), axis=0)) * REPLICAS ** (-0.5)
    mean_down = lax.optimization_barrier(jnp.sum(partial_down.astype(jnp.float32), axis=0)) * REPLICAS ** (-0.5)
    mean_norm = lax.optimization_barrier(jnp.sum(partial_norm.astype(jnp.float32), axis=0)) * REPLICAS ** (-0.5)
    ratio_gate = jnp.sqrt(lax.optimization_barrier(jnp.sum(master_gate * master_gate, axis=1, keepdims=True))) * lax.rsqrt(lax.optimization_barrier(jnp.sum(mean_gate * mean_gate, axis=1, keepdims=True)) + 1e-06)
    mean_gate = mean_gate * ratio_gate
    ratio_up = jnp.sqrt(lax.optimization_barrier(jnp.sum(master_up * master_up, axis=1, keepdims=True))) * lax.rsqrt(lax.optimization_barrier(jnp.sum(mean_up * mean_up, axis=1, keepdims=True)) + 1e-06)
    mean_up = mean_up * ratio_up
    ratio_down = jnp.sqrt(lax.optimization_barrier(jnp.sum(master_down * master_down, axis=0, keepdims=True))) * lax.rsqrt(lax.optimization_barrier(jnp.sum(mean_down * mean_down, axis=0, keepdims=True)) + 1e-06)
    mean_down = mean_down * ratio_down
    state_new_gate = hold_rate * memory_gate + mean_gate
    stepped_gate = master_gate - learn_rate * state_new_gate
    state_new_up = hold_rate * memory_up + mean_up
    stepped_up = master_up - learn_rate * state_new_up
    state_new_down = hold_rate * memory_down + mean_down
    stepped_down = master_down - learn_rate * state_new_down
    state_new_norm = hold_rate * memory_norm + mean_norm
    stepped_norm = master_norm - learn_rate * state_new_norm
    compute_gate = stepped_gate.astype(jnp.bfloat16)
    compute_up = stepped_up.astype(jnp.bfloat16)
    compute_down = stepped_down.astype(jnp.bfloat16)
    compute_norm = stepped_norm.astype(jnp.bfloat16)
    return (compute_gate, compute_up, compute_down, compute_norm, stepped_gate, stepped_up, stepped_down, stepped_norm, state_new_gate, state_new_up, state_new_down, state_new_norm)
```

```python
import functools
import math

import jax
import jax.numpy as jnp
from jax import lax
from jax.experimental import pallas as pl
from jax.experimental.pallas import tpu as pltpu
from jax.sharding import PartitionSpec as P

learn_rate = 0.5
hold_rate = 0.9
MESH = pl.DeviceIdType.MESH
LANES = 128


def cut(ref, axis, start, size):
    return ref.at[pl.ds(start, size), :] if axis == 0 else ref.at[:, pl.ds(start, size)]


def kernel(n, m, axes, *refs):
    refs = list(refs)
    take = lambda count: [refs.pop(0) for _ in range(count)]
    t = len(axes)
    partial, (partial_norm,) = take(t), take(1)
    master_hbm, (master_norm,) = take(t), take(1)
    memory_hbm, (memory_norm,) = take(t), take(1)
    compute, (compute_norm,) = take(t), take(1)
    stepped, (stepped_norm,) = take(t), take(1)
    state, (state_norm,) = take(t), take(1)
    got, memory = take(t), take(t)
    master, mean = stepped, state
    mean_n, got_n, master_n, memory_n, whole_n, line_n = take(6)
    own_line, own_got, slope_line, slope_got, fold, tile = take(6)
    load_sem, norm_load_sem = take(2)
    part_send, part_recv, comp_send, comp_recv = take(4)
    own_send, own_recv, slope_send, slope_recv = take(4)
    pn_send, pn_recv, wn_send, wn_recv = take(4)

    me = lax.axis_index("replica")
    at = lax.axis_index("model")
    rate = n ** (-0.5)
    peers = [lax.rem(me + k, n) for k in range(1, n)]
    mates = [lax.rem(at + k, m) for k in range(1, m)]

    chunks = []
    for which, axis in enumerate(axes):
        share = mean[which].shape[axis]
        chunks += [(which, c) for c in range(share // LANES)]
    count = len(chunks)

    def load(kind, number):
        which, c = chunks[number]
        axis = axes[which]
        share = mean[which].shape[axis]
        if kind == 0:
            source = cut(master_hbm[which], axis, c * LANES, LANES)
            target = master[which]
        elif kind == 1:
            start = pl.multiple_of(me * share + c * LANES, LANES)
            source = cut(partial[which].at[0], axis, start, LANES)
            target = mean[which]
        else:
            source = cut(memory_hbm[which], axis, c * LANES, LANES)
            target = memory[which]
        return pltpu.make_async_copy(
            source, cut(target, axis, c * LANES, LANES), load_sem.at[kind, number]
        )

    share_n = mean_n.shape[1]
    norm_loads = [
        pltpu.make_async_copy(
            partial_norm.at[:, pl.ds(pl.multiple_of(me * share_n, LANES), share_n)],
            mean_n,
            norm_load_sem.at[0],
        ),
        pltpu.make_async_copy(master_norm, master_n, norm_load_sem.at[1]),
        pltpu.make_async_copy(memory_norm, memory_n, norm_load_sem.at[2]),
    ]
    barrier = pltpu.get_barrier_semaphore()
    for peer in peers:
        pl.semaphore_signal(barrier, inc=1, device_id={"replica": peer}, device_id_type=MESH)
    for mate in mates:
        pl.semaphore_signal(barrier, inc=1, device_id={"model": mate}, device_id_type=MESH)
    for kind in range(3):
        for number in range(count):
            load(kind, number).start()
    for copy in norm_loads:
        copy.start()
    pl.semaphore_wait(barrier, n - 1 + m - 1)

    def part_copy(number, k):
        which, c = chunks[number]
        axis = axes[which]
        share = mean[which].shape[axis]
        start = pl.multiple_of(peers[k] * share + c * LANES, LANES)
        return pltpu.make_async_remote_copy(
            src_ref=cut(partial[which].at[0], axis, start, LANES),
            dst_ref=cut(got[which].at[k], axis, c * LANES, LANES),
            send_sem=part_send.at[number, k],
            recv_sem=part_recv.at[number, k],
            device_id={"replica": peers[k]},
            device_id_type=MESH,
        )

    def pn_copy(k):
        return pltpu.make_async_remote_copy(
            src_ref=partial_norm.at[
                :, pl.ds(pl.multiple_of(peers[k] * share_n, LANES), share_n)
            ],
            dst_ref=got_n.at[k],
            send_sem=pn_send.at[k],
            recv_sem=pn_recv.at[k],
            device_id={"replica": peers[k]},
            device_id_type=MESH,
        )

    for k in range(n - 1):
        pn_copy(k).start()
    for number in range(count):
        for k in range(n - 1):
            part_copy(number, k).start()

    def folded(square):
        return sum(
            square[:, j : j + LANES] for j in range(0, square.shape[1], LANES)
        )

    def line_of(number, block_of, rows, keep):
        which, c = chunks[number]
        if axes[which] == 0:
            height = 32
            for b in range(LANES // height):
                value = block_of(pl.ds(c * LANES + b * height, height), slice(None))
                if keep is not None:
                    keep[pl.ds(c * LANES + b * height, height), :] = value
                fold[pl.ds(b * height, height), :] = folded(value * value)
            return jnp.sum(fold[...].T, axis=0, keepdims=True)
        height = next(h for h in (128, 64, 32, 16, 8) if rows % h == 0)
        total = jnp.zeros((8, LANES), jnp.float32)
        lanes = pl.ds(c * LANES, LANES)
        for b in range(rows // height):
            value = block_of(pl.ds(b * height, height), lanes)
            if keep is not None:
                keep[pl.ds(b * height, height), lanes] = value
            total = total + jnp.sum((value * value).reshape(height // 8, 8, LANES), axis=0)
        return jnp.sum(total, axis=0, keepdims=True)

    def own_copy(k):
        return pltpu.make_async_remote_copy(
            src_ref=own_line,
            dst_ref=own_got.at[k],
            send_sem=own_send.at[k],
            recv_sem=own_recv.at[k],
            device_id={"model": mates[k]},
            device_id_type=MESH,
        )

    for number in range(count):
        which, c = chunks[number]
        load(0, number).wait()
        own_line[number] = line_of(
            number, lambda r, l: master[which][r, l], master[which].shape[0], None
        )
    for k in range(m - 1):
        own_copy(k).start()

    def wn_copy(k):
        mine = whole_n.at[:, pl.ds(pl.multiple_of(me * share_n, LANES), share_n)]
        return pltpu.make_async_remote_copy(
            src_ref=mine,
            dst_ref=mine,
            send_sem=wn_send.at[k],
            recv_sem=wn_recv.at[k],
            device_id={"replica": peers[k]},
            device_id_type=MESH,
        )

    for copy in norm_loads:
        copy.wait()
    total = mean_n[...]
    for k in range(n - 1):
        pn_copy(k).wait()
        total = total + got_n[k]
    new = hold_rate * memory_n[...] + total * rate
    state_norm[...] = new
    new = master_n[...] - learn_rate * new
    stepped_norm[...] = new
    whole_n[:, pl.ds(pl.multiple_of(me * share_n, LANES), share_n)] = new
    for k in range(n - 1):
        wn_copy(k).start()

    def slope_copy(number, k):
        return pltpu.make_async_remote_copy(
            src_ref=slope_line.at[number],
            dst_ref=slope_got.at[number, k],
            send_sem=slope_send.at[number, k],
            recv_sem=slope_recv.at[number, k],
            device_id={"model": mates[k]},
            device_id_type=MESH,
        )

    def reduce(number):
        which, c = chunks[number]
        load(1, number).wait()
        for k in range(n - 1):
            part_copy(number, k).wait_recv()

        def block(r, l):
            value = mean[which][r, l]
            for k in range(n - 1):
                value = value + got[which][k, r, l]
            return value * rate

        slope_line[number] = line_of(number, block, mean[which].shape[0], mean[which])
        for k in range(m - 1):
            slope_copy(number, k).start()

    def comp_copy(number, k):
        which, c = chunks[number]
        axis = axes[which]
        share = mean[which].shape[axis]
        mine = cut(compute[which], axis, pl.multiple_of(me * share + c * LANES, LANES), LANES)
        return pltpu.make_async_remote_copy(
            src_ref=mine,
            dst_ref=mine,
            send_sem=comp_send.at[number, k],
            recv_sem=comp_recv.at[number, k],
            device_id={"replica": peers[k]},
            device_id_type=MESH,
        )

    def update(number):
        which, c = chunks[number]
        axis = axes[which]
        share = mean[which].shape[axis]
        own, slope = own_line[number], slope_line[number]
        for k in range(m - 1):
            slope_copy(number, k).wait_recv()
            own = own + own_got[k, number]
            slope = slope + slope_got[number, k]
        ratio = jnp.sqrt(own) * lax.rsqrt(slope + 1e-06)
        load(2, number).wait()
        base = pl.multiple_of(me * share, LANES)

        def finish(r, l, r_out, l_out, scale):
            new = hold_rate * memory[which][r, l] + mean[which][r, l] * scale
            state[which][r, l] = new
            new = master[which][r, l] - learn_rate * new
            stepped[which][r, l] = new
            compute[which][r_out, l_out] = new.astype(jnp.bfloat16)

        if axis == 0:
            tile[...] = jnp.broadcast_to(ratio, (LANES, LANES)).T
            height, width = 32, mean[which].shape[1]
            for b in range(LANES // height):
                first = c * LANES + b * height
                finish(
                    pl.ds(first, height),
                    slice(None),
                    pl.ds(pl.multiple_of(base + first, height), height),
                    slice(None),
                    jnp.concatenate(
                        [tile[pl.ds(b * height, height), :]] * (width // LANES), axis=1
                    ),
                )
        else:
            rows = mean[which].shape[0]
            height = next(h for h in (128, 64, 32, 16, 8) if rows % h == 0)
            for b in range(rows // height):
                r = pl.ds(b * height, height)
                finish(
                    r,
                    pl.ds(c * LANES, LANES),
                    r,
                    pl.ds(pl.multiple_of(base + c * LANES, LANES), LANES),
                    ratio,
                )
        for k in range(n - 1):
            comp_copy(number, k).start()

    ahead = 4
    for number in range(count + ahead):
        if number < count:
            reduce(number)
        if number == ahead:
            for k in range(m - 1):
                own_copy(k).wait()
        if number >= ahead:
            update(number - ahead)

    for k in range(n - 1):
        wn_copy(k).wait()
    for j in range(whole_n.shape[1] // LANES):
        line_n[pl.ds(j, 1), :] = whole_n[:, j * LANES : (j + 1) * LANES]
    compute_norm[...] = line_n[...].astype(jnp.bfloat16)
    for number in range(count):
        for k in range(n - 1):
            part_copy(number, k).wait_send()
            comp_copy(number, k).wait()
        for k in range(m - 1):
            slope_copy(number, k).wait_send()


def drain(*refs):
    half = len(refs) // 2
    sems = refs[-1]
    copies = [
        pltpu.make_async_copy(refs[i], refs[half + i], sems.at[i]) for i in range(half)
    ]
    for copy in copies:
        copy.start()
    for copy in copies:
        copy.wait()


def exchange(n, m, args):
    axes = (0, 0, 1)
    partial, partial_norm = args[0:3], args[3]
    master, master_norm = args[4:7], args[7]
    memory, memory_norm = args[8:11], args[11]
    row = lambda x: x.reshape(1, -1)
    shapes = [x.shape for x in master]
    count = sum(s[a] // LANES for s, a in zip(shapes, axes))
    share_n, width_n = master_norm.shape[0], partial_norm.shape[1]
    f32, bf16 = jnp.float32, jnp.bfloat16
    dma = lambda *s: pltpu.SemaphoreType.DMA(s)
    out_shape = (
        [pltpu.VMEM(x.shape[1:], bf16) for x in partial]
        + [pltpu.VMEM((width_n // LANES, LANES), bf16)]
        + ([pltpu.VMEM(s, f32) for s in shapes] + [pltpu.VMEM((1, share_n), f32)]) * 2
    )
    scratch = (
        [pltpu.VMEM((n - 1,) + s, f32) for s in shapes]
        + [pltpu.VMEM(s, f32) for s in shapes]
        + [
            pltpu.VMEM((1, share_n), f32),
            pltpu.VMEM((n - 1, 1, share_n), f32),
            pltpu.VMEM((1, share_n), f32),
            pltpu.VMEM((1, share_n), f32),
            pltpu.VMEM((1, width_n), f32),
            pltpu.VMEM((width_n // LANES, LANES), f32),
            pltpu.VMEM((count, 1, LANES), f32),
            pltpu.VMEM((m - 1, count, 1, LANES), f32),
            pltpu.VMEM((count, 1, LANES), f32),
            pltpu.VMEM((count, m - 1, 1, LANES), f32),
            pltpu.VMEM((LANES, LANES), f32),
            pltpu.VMEM((LANES, LANES), f32),
            dma(3, count),
            dma(3),
        ]
        + [dma(count, n - 1)] * 4
        + [dma(m - 1)] * 2
        + [dma(count, m - 1)] * 2
        + [dma(n - 1)] * 4
    )
    results = sum(math.prod(x.shape) * jnp.dtype(x.dtype).itemsize for x in out_shape)
    room = 63 * 2**20 - results
    outs = pl.pallas_call(
        functools.partial(kernel, n, m, axes),
        out_shape=out_shape,
        in_specs=[pl.BlockSpec(memory_space=pltpu.HBM)] * 12,
        out_specs=[pl.BlockSpec(memory_space=pltpu.VMEM)] * 12,
        scratch_shapes=scratch,
        compiler_params=pltpu.CompilerParams(
            collective_id=0, has_side_effects=True, vmem_limit_bytes=room
        ),
    )(
        *partial, partial_norm, *master, row(master_norm), *memory, row(memory_norm)
    )
    outs = pl.pallas_call(
        drain,
        out_shape=[jax.ShapeDtypeStruct(x.shape, x.dtype) for x in outs],
        in_specs=[pl.BlockSpec(memory_space=pl.ANY)] * len(outs),
        out_specs=[pl.BlockSpec(memory_space=pltpu.HBM)] * len(outs),
        scratch_shapes=[dma(len(outs))],
        compiler_params=pltpu.CompilerParams(vmem_limit_bytes=2**20),
    )(*outs)
    return [x.reshape(-1) if i % 4 == 3 else x for i, x in enumerate(outs)]


def plain(args):
    partial, master, memory = args[0:4], args[4:8], args[8:12]
    n = lax.axis_size("replica")
    axes = (0, 0, 1, 0)
    mean = [
        lax.psum_scatter(p[0], "replica", scatter_dimension=a, tiled=True) * n ** (-0.5)
        for p, a in zip(partial, axes)
    ]
    square = lambda x, a: jnp.sum(x * x, axis=1 - a, keepdims=True)
    own, slope = lax.psum(
        (
            [square(x, a) for x, a in zip(master[:3], axes)],
            [square(x, a) for x, a in zip(mean[:3], axes)],
        ),
        "model",
    )
    mean = [
        x * (jnp.sqrt(o) * lax.rsqrt(s + 1e-06)) for x, o, s in zip(mean[:3], own, slope)
    ] + mean[3:]
    state = [hold_rate * e + x for e, x in zip(memory, mean)]
    stepped = [w - learn_rate * s for w, s in zip(master, state)]
    compute = [
        lax.all_gather(s.astype(jnp.bfloat16), "replica", axis=a, tiled=True)
        for s, a in zip(stepped, axes)
    ]
    return compute + stepped + state


def on_device(*args):
    n, m = lax.axis_size("replica"), lax.axis_size("model")
    shares = (args[4].shape[0], args[5].shape[0], args[6].shape[1], args[7].shape[0])
    if n > 1 and m > 1 and all(s % LANES == 0 for s in shares):
        return tuple(exchange(n, m, args))
    return tuple(plain(args))


def solution(mesh):
    partial = P(("shift", "replica"), None, "model")
    rows, columns = P(("shift", "replica"), "model"), P(("shift", "model"), "replica")
    vector = P(("shift", "replica"))
    own = (rows, rows, columns, vector)
    return jax.shard_map(
        on_device,
        mesh=mesh,
        in_specs=(
            partial,
            partial,
            P(("shift", "replica"), "model", None),
            P(("shift", "replica"), None),
        )
        + own
        + own,
        out_specs=(
            P("shift", "model"),
            P("shift", "model"),
            P(("shift", "model"), None),
            P("shift"),
        )
        + own
        + own,
        check_vma=False,
    )
```

```python
import functools
import math

import jax
import jax.numpy as jnp
from jax import lax
from jax.experimental import pallas as pl
from jax.experimental.pallas import tpu as pltpu
from jax.sharding import PartitionSpec as P

learn_rate = 0.5
hold_rate = 0.9
MESH = pl.DeviceIdType.MESH
LANES = 128


def cut(ref, axis, start, size):
    return ref.at[pl.ds(start, size), :] if axis == 0 else ref.at[:, pl.ds(start, size)]


def kernel(n, m, axes, *refs):
    refs = list(refs)
    take = lambda count: [refs.pop(0) for _ in range(count)]
    t = len(axes)
    partial, (partial_norm,) = take(t), take(1)
    master_hbm, (master_norm,) = take(t), take(1)
    memory_hbm, (memory_norm,) = take(t), take(1)
    compute, (compute_norm,) = take(t), take(1)
    stepped, (stepped_norm,) = take(t), take(1)
    state, (state_norm,) = take(t), take(1)
    got, memory = take(t), take(t)
    master, mean = stepped, state
    mean_n, got_n, master_n, memory_n, whole_n, line_n = take(6)
    own_line, own_got, slope_line, slope_got, fold, tile = take(6)
    load_sem, norm_load_sem = take(2)
    part_send, part_recv, comp_send, comp_recv = take(4)
    own_send, own_recv, slope_send, slope_recv = take(4)
    pn_send, pn_recv, wn_send, wn_recv = take(4)

    me = lax.axis_index("replica")
    at = lax.axis_index("model")
    rate = n ** (-0.5)
    peers = [lax.rem(me + k, n) for k in range(1, n)]
    mates = [lax.rem(at + k, m) for k in range(1, m)]

    chunks = []
    for which, axis in enumerate(axes):
        share = mean[which].shape[axis]
        chunks += [(which, c) for c in range(share // LANES)]
    count = len(chunks)

    def load(kind, number):
        which, c = chunks[number]
        axis = axes[which]
        share = mean[which].shape[axis]
        if kind == 0:
            source = cut(master_hbm[which], axis, c * LANES, LANES)
            target = master[which]
        elif kind == 1:
            start = pl.multiple_of(me * share + c * LANES, LANES)
            source = cut(partial[which].at[0], axis, start, LANES)
            target = mean[which]
        else:
            source = cut(memory_hbm[which], axis, c * LANES, LANES)
            target = memory[which]
        return pltpu.make_async_copy(
            source, cut(target, axis, c * LANES, LANES), load_sem.at[kind, number]
        )

    share_n = mean_n.shape[1]
    norm_loads = [
        pltpu.make_async_copy(
            partial_norm.at[:, pl.ds(pl.multiple_of(me * share_n, LANES), share_n)],
            mean_n,
            norm_load_sem.at[0],
        ),
        pltpu.make_async_copy(master_norm, master_n, norm_load_sem.at[1]),
        pltpu.make_async_copy(memory_norm, memory_n, norm_load_sem.at[2]),
    ]
    barrier = pltpu.get_barrier_semaphore()
    for peer in peers:
        pl.semaphore_signal(barrier, inc=1, device_id={"replica": peer}, device_id_type=MESH)
    for mate in mates:
        pl.semaphore_signal(barrier, inc=1, device_id={"model": mate}, device_id_type=MESH)
    for kind in range(3):
        for number in range(count):
            load(kind, number).start()
    for copy in norm_loads:
        copy.start()
    pl.semaphore_wait(barrier, n - 1 + m - 1)

    def part_copy(number, k):
        which, c = chunks[number]
        axis = axes[which]
        share = mean[which].shape[axis]
        start = pl.multiple_of(peers[k] * share + c * LANES, LANES)
        return pltpu.make_async_remote_copy(
            src_ref=cut(partial[which].at[0], axis, start, LANES),
            dst_ref=cut(got[which].at[k], axis, c * LANES, LANES),
            send_sem=part_send.at[number, k],
            recv_sem=part_recv.at[number, k],
            device_id={"replica": peers[k]},
            device_id_type=MESH,
        )

    def pn_copy(k):
        return pltpu.make_async_remote_copy(
            src_ref=partial_norm.at[
                :, pl.ds(pl.multiple_of(peers[k] * share_n, LANES), share_n)
            ],
            dst_ref=got_n.at[k],
            send_sem=pn_send.at[k],
            recv_sem=pn_recv.at[k],
            device_id={"replica": peers[k]},
            device_id_type=MESH,
        )

    for k in range(n - 1):
        pn_copy(k).start()
    for number in range(count):
        for k in range(n - 1):
            part_copy(number, k).start()

    def folded(square):
        return sum(
            square[:, j : j + LANES] for j in range(0, square.shape[1], LANES)
        )

    def line_of(number, block_of, rows, keep):
        which, c = chunks[number]
        if axes[which] == 0:
            height = 32
            for b in range(LANES // height):
                value = block_of(pl.ds(c * LANES + b * height, height), slice(None))
                if keep is not None:
                    keep[pl.ds(c * LANES + b * height, height), :] = value
                fold[pl.ds(b * height, height), :] = folded(value * value)
            return jnp.sum(fold[...].T, axis=0, keepdims=True)
        height = next(h for h in (128, 64, 32, 16, 8) if rows % h == 0)
        total = jnp.zeros((8, LANES), jnp.float32)
        lanes = pl.ds(c * LANES, LANES)
        for b in range(rows // height):
            value = block_of(pl.ds(b * height, height), lanes)
            if keep is not None:
                keep[pl.ds(b * height, height), lanes] = value
            total = total + jnp.sum((value * value).reshape(height // 8, 8, LANES), axis=0)
        return jnp.sum(total, axis=0, keepdims=True)

    def own_copy(k):
        return pltpu.make_async_remote_copy(
            src_ref=own_line,
            dst_ref=own_got.at[k],
            send_sem=own_send.at[k],
            recv_sem=own_recv.at[k],
            device_id={"model": mates[k]},
            device_id_type=MESH,
        )

    for number in range(count):
        which, c = chunks[number]
        load(0, number).wait()
        own_line[number] = line_of(
            number, lambda r, l: master[which][r, l], master[which].shape[0], None
        )
    for k in range(m - 1):
        own_copy(k).start()

    def wn_copy(k):
        mine = whole_n.at[:, pl.ds(pl.multiple_of(me * share_n, LANES), share_n)]
        return pltpu.make_async_remote_copy(
            src_ref=mine,
            dst_ref=mine,
            send_sem=wn_send.at[k],
            recv_sem=wn_recv.at[k],
            device_id={"replica": peers[k]},
            device_id_type=MESH,
        )

    for copy in norm_loads:
        copy.wait()
    total = mean_n[...]
    for k in range(n - 1):
        pn_copy(k).wait()
        total = total + got_n[k]
    new = hold_rate * memory_n[...] + total * rate
    state_norm[...] = new
    new = master_n[...] - learn_rate * new
    stepped_norm[...] = new
    whole_n[:, pl.ds(pl.multiple_of(me * share_n, LANES), share_n)] = new
    for k in range(n - 1):
        wn_copy(k).start()

    def slope_copy(number, k):
        return pltpu.make_async_remote_copy(
            src_ref=slope_line.at[number],
            dst_ref=slope_got.at[number, k],
            send_sem=slope_send.at[number, k],
            recv_sem=slope_recv.at[number, k],
            device_id={"model": mates[k]},
            device_id_type=MESH,
        )

    def reduce(number):
        which, c = chunks[number]
        load(1, number).wait()
        for k in range(n - 1):
            part_copy(number, k).wait_recv()

        def block(r, l):
            value = mean[which][r, l]
            for k in range(n - 1):
                value = value + got[which][k, r, l]
            return value * rate

        slope_line[number] = line_of(number, block, mean[which].shape[0], mean[which])
        for k in range(m - 1):
            slope_copy(number, k).start()

    def comp_copy(number, k):
        which, c = chunks[number]
        axis = axes[which]
        share = mean[which].shape[axis]
        mine = cut(compute[which], axis, pl.multiple_of(me * share + c * LANES, LANES), LANES)
        return pltpu.make_async_remote_copy(
            src_ref=mine,
            dst_ref=mine,
            send_sem=comp_send.at[number, k],
            recv_sem=comp_recv.at[number, k],
            device_id={"replica": peers[k]},
            device_id_type=MESH,
        )

    def update(number):
        which, c = chunks[number]
        axis = axes[which]
        share = mean[which].shape[axis]
        own, slope = own_line[number], slope_line[number]
        for k in range(m - 1):
            slope_copy(number, k).wait_recv()
            own = own + own_got[k, number]
            slope = slope + slope_got[number, k]
        ratio = jnp.sqrt(own) * lax.rsqrt(slope + 1e-06)
        load(2, number).wait()
        base = pl.multiple_of(me * share, LANES)

        def finish(r, l, r_out, l_out, scale):
            new = hold_rate * memory[which][r, l] + mean[which][r, l] * scale
            state[which][r, l] = new
            new = master[which][r, l] - learn_rate * new
            stepped[which][r, l] = new
            compute[which][r_out, l_out] = new.astype(jnp.bfloat16)

        if axis == 0:
            tile[...] = jnp.broadcast_to(ratio, (LANES, LANES)).T
            height, width = 32, mean[which].shape[1]
            for b in range(LANES // height):
                first = c * LANES + b * height
                finish(
                    pl.ds(first, height),
                    slice(None),
                    pl.ds(pl.multiple_of(base + first, height), height),
                    slice(None),
                    jnp.concatenate(
                        [tile[pl.ds(b * height, height), :]] * (width // LANES), axis=1
                    ),
                )
        else:
            rows = mean[which].shape[0]
            height = next(h for h in (128, 64, 32, 16, 8) if rows % h == 0)
            for b in range(rows // height):
                r = pl.ds(b * height, height)
                finish(
                    r,
                    pl.ds(c * LANES, LANES),
                    r,
                    pl.ds(pl.multiple_of(base + c * LANES, LANES), LANES),
                    ratio,
                )
        for k in range(n - 1):
            comp_copy(number, k).start()

    ahead = 8
    for number in range(count + ahead):
        if number < count:
            reduce(number)
        if number == ahead:
            for k in range(m - 1):
                own_copy(k).wait()
        if number >= ahead:
            update(number - ahead)

    for k in range(n - 1):
        wn_copy(k).wait()
    for j in range(whole_n.shape[1] // LANES):
        line_n[pl.ds(j, 1), :] = whole_n[:, j * LANES : (j + 1) * LANES]
    compute_norm[...] = line_n[...].astype(jnp.bfloat16)
    for number in range(count):
        for k in range(n - 1):
            part_copy(number, k).wait_send()
            comp_copy(number, k).wait()
        for k in range(m - 1):
            slope_copy(number, k).wait_send()


def drain(*refs):
    half = len(refs) // 2
    sems = refs[-1]
    copies = [
        pltpu.make_async_copy(refs[i], refs[half + i], sems.at[i]) for i in range(half)
    ]
    for copy in copies:
        copy.start()
    for copy in copies:
        copy.wait()


def exchange(n, m, args):
    axes = (0, 0, 1)
    partial, partial_norm = args[0:3], args[3]
    master, master_norm = args[4:7], args[7]
    memory, memory_norm = args[8:11], args[11]
    row = lambda x: x.reshape(1, -1)
    shapes = [x.shape for x in master]
    count = sum(s[a] // LANES for s, a in zip(shapes, axes))
    share_n, width_n = master_norm.shape[0], partial_norm.shape[1]
    f32, bf16 = jnp.float32, jnp.bfloat16
    dma = lambda *s: pltpu.SemaphoreType.DMA(s)
    out_shape = (
        [pltpu.VMEM(x.shape[1:], bf16) for x in partial]
        + [pltpu.VMEM((width_n // LANES, LANES), bf16)]
        + ([pltpu.VMEM(s, f32) for s in shapes] + [pltpu.VMEM((1, share_n), f32)]) * 2
    )
    scratch = (
        [pltpu.VMEM((n - 1,) + s, f32) for s in shapes]
        + [pltpu.VMEM(s, f32) for s in shapes]
        + [
            pltpu.VMEM((1, share_n), f32),
            pltpu.VMEM((n - 1, 1, share_n), f32),
            pltpu.VMEM((1, share_n), f32),
            pltpu.VMEM((1, share_n), f32),
            pltpu.VMEM((1, width_n), f32),
            pltpu.VMEM((width_n // LANES, LANES), f32),
            pltpu.VMEM((count, 1, LANES), f32),
            pltpu.VMEM((m - 1, count, 1, LANES), f32),
            pltpu.VMEM((count, 1, LANES), f32),
            pltpu.VMEM((count, m - 1, 1, LANES), f32),
            pltpu.VMEM((LANES, LANES), f32),
            pltpu.VMEM((LANES, LANES), f32),
            dma(3, count),
            dma(3),
        ]
        + [dma(count, n - 1)] * 4
        + [dma(m - 1)] * 2
        + [dma(count, m - 1)] * 2
        + [dma(n - 1)] * 4
    )
    results = sum(math.prod(x.shape) * jnp.dtype(x.dtype).itemsize for x in out_shape)
    room = 63 * 2**20 - results
    outs = pl.pallas_call(
        functools.partial(kernel, n, m, axes),
        out_shape=out_shape,
        in_specs=[pl.BlockSpec(memory_space=pltpu.HBM)] * 12,
        out_specs=[pl.BlockSpec(memory_space=pltpu.VMEM)] * 12,
        scratch_shapes=scratch,
        compiler_params=pltpu.CompilerParams(
            collective_id=0, has_side_effects=True, vmem_limit_bytes=room
        ),
    )(
        *partial, partial_norm, *master, row(master_norm), *memory, row(memory_norm)
    )
    outs = pl.pallas_call(
        drain,
        out_shape=[jax.ShapeDtypeStruct(x.shape, x.dtype) for x in outs],
        in_specs=[pl.BlockSpec(memory_space=pl.ANY)] * len(outs),
        out_specs=[pl.BlockSpec(memory_space=pltpu.HBM)] * len(outs),
        scratch_shapes=[dma(len(outs))],
        compiler_params=pltpu.CompilerParams(vmem_limit_bytes=2**20),
    )(*outs)
    return [x.reshape(-1) if i % 4 == 3 else x for i, x in enumerate(outs)]


def plain(args):
    partial, master, memory = args[0:4], args[4:8], args[8:12]
    n = lax.axis_size("replica")
    axes = (0, 0, 1, 0)
    mean = [
        lax.psum_scatter(p[0], "replica", scatter_dimension=a, tiled=True) * n ** (-0.5)
        for p, a in zip(partial, axes)
    ]
    square = lambda x, a: jnp.sum(x * x, axis=1 - a, keepdims=True)
    own, slope = lax.psum(
        (
            [square(x, a) for x, a in zip(master[:3], axes)],
            [square(x, a) for x, a in zip(mean[:3], axes)],
        ),
        "model",
    )
    mean = [
        x * (jnp.sqrt(o) * lax.rsqrt(s + 1e-06)) for x, o, s in zip(mean[:3], own, slope)
    ] + mean[3:]
    state = [hold_rate * e + x for e, x in zip(memory, mean)]
    stepped = [w - learn_rate * s for w, s in zip(master, state)]
    compute = [
        lax.all_gather(s.astype(jnp.bfloat16), "replica", axis=a, tiled=True)
        for s, a in zip(stepped, axes)
    ]
    return compute + stepped + state


def on_device(*args):
    n, m = lax.axis_size("replica"), lax.axis_size("model")
    shares = (args[4].shape[0], args[5].shape[0], args[6].shape[1], args[7].shape[0])
    if n > 1 and m > 1 and all(s % LANES == 0 for s in shares):
        return tuple(exchange(n, m, args))
    return tuple(plain(args))


def solution(mesh):
    partial = P(("shift", "replica"), None, "model")
    rows, columns = P(("shift", "replica"), "model"), P(("shift", "model"), "replica")
    vector = P(("shift", "replica"))
    own = (rows, rows, columns, vector)
    return jax.shard_map(
        on_device,
        mesh=mesh,
        in_specs=(
            partial,
            partial,
            P(("shift", "replica"), "model", None),
            P(("shift", "replica"), None),
        )
        + own
        + own,
        out_specs=(
            P("shift", "model"),
            P("shift", "model"),
            P(("shift", "model"), None),
            P("shift"),
        )
        + own
        + own,
        check_vma=False,
    )
```
